8 devices in a mesh: fsdp: 8 (over z, y, x, core).
Axes of the slice: x: 2, y: 2, z: 1, core: 2. Of those that a mesh axis runs over, the one named last changes fastest.
Arguments:
- grad_mat: bfloat16 [8, 29491200], P('fsdp')
- grad_vec: bfloat16 [8, 11264], P('fsdp')
- master_mat: float32 [29491200], P('fsdp')
- moment_mat: float32 [29491200], P('fsdp')
- second_mat: float32 [29491200], P('fsdp')
- master_vec: float32 [11264], P('fsdp')
- moment_vec: float32 [11264], P('fsdp')
- second_vec: float32 [11264], P('fsdp')
Outputs:
- output 1: float32 [29491200], P('fsdp')
- output 2: float32 [29491200], P('fsdp')
- output 3: float32 [29491200], P('fsdp')
- output 4: float32 [11264], P('fsdp')
- output 5: float32 [11264], P('fsdp')
- output 6: float32 [11264], P('fsdp')
- output 7: bfloat16 [29491200], replicated
- output 8: bfloat16 [11264], replicated
All inputs are finite; a program needn't handle non-finite values.
Results may differ from the reference program's by a relative error of at most 0.001.
Values are sent between devices in bfloat16 or wider.
A program may use at most 1 GiB of HBM per device.

```python
import jax
import jax.numpy as jnp
from jax import lax

D = 960
HEADS = 15
KV_HEADS = 5
HEAD = 64
FF = 2560
LAYERS = 3
GROUP = 8
NM_PAD = 29491200
NV_PAD = 11264
STEP = 4

Q_OUT = HEADS * HEAD
KV_OUT = KV_HEADS * HEAD
MAT_COUNT = LAYERS * (2 * D * Q_OUT + 2 * D * KV_OUT + 3 * D * FF)
VEC_COUNT = LAYERS * (Q_OUT + 2 * KV_OUT + 2 * D)
GRAD_UNIT = (MAT_COUNT + VEC_COUNT) ** -0.5
TARGET_NORM = 3.0
LEARN_RATE = 1e-3
BETA_ONE = 0.9
BETA_TWO = 0.999
ADAM_EPS = 1e-8
DECAY = 0.01
NORM_EPS = 1e-6
FIX_ONE = 1.0 - BETA_ONE ** STEP
FIX_TWO = 1.0 - BETA_TWO ** STEP


def pad_flat(flat, total):
    return jnp.pad(flat, (0, total - flat.shape[0]))


def layer_draw(key, pieces):
    sub_keys = jax.random.split(key, len(pieces))
    drawn = [jax.random.normal(sub_key, (LAYERS, length), jnp.float32) * scale + offset
             for sub_key, (length, scale, offset) in zip(sub_keys, pieces)]
    return jnp.concatenate(drawn, axis=1).reshape(-1)


def grad_rows(key, total, valid):
    keep = jnp.arange(total) < valid
    scale = TARGET_NORM * GRAD_UNIT * GROUP ** -0.5

    def one_row(row):
        noise = jax.random.normal(jax.random.fold_in(key, row), (total,), jnp.float32)
        return jnp.where(keep, noise * scale, 0.0).astype(jnp.bfloat16)

    return lax.map(one_row, jnp.arange(GROUP))


def moment_draw(key, total, valid):
    keep = jnp.arange(total) < valid
    noise = jax.random.normal(key, (total,), jnp.float32)
    return jnp.where(keep, 0.1 * GRAD_UNIT * noise, 0.0)


def second_draw(key, total, valid):
    keep = jnp.arange(total) < valid
    noise = jax.random.normal(key, (total,), jnp.float32)
    return jnp.where(keep, 0.003 * GRAD_UNIT ** 2 * (noise * noise + 0.5), 0.0)


def setup_inputs(seed: int = 0) -> dict:
    keys = jax.random.split(jax.random.key(seed), 8)
    mat_pieces = [(D * Q_OUT, D ** -0.5, 0.0), (D * KV_OUT, D ** -0.5, 0.0), (D * KV_OUT, D ** -0.5, 0.0),
                  (Q_OUT * D, Q_OUT ** -0.5, 0.0), (D * FF, D ** -0.5, 0.0), (D * FF, D ** -0.5, 0.0),
                  (FF * D, FF ** -0.5, 0.0)]
    vec_pieces = [(Q_OUT, 0.5, 0.0), (KV_OUT, 0.5, 0.0), (KV_OUT, 0.5, 0.0), (D, 0.2, 1.0), (D, 0.2, 1.0)]
    return {
        'grad_mat': grad_rows(keys[0], NM_PAD, MAT_COUNT),
        'grad_vec': grad_rows(keys[1], NV_PAD, VEC_COUNT),
        'master_mat': pad_flat(layer_draw(keys[2], mat_pieces), NM_PAD),
        'moment_mat': moment_draw(keys[3], NM_PAD, MAT_COUNT),
        'second_mat': second_draw(keys[4], NM_PAD, MAT_COUNT),
        'master_vec': pad_flat(layer_draw(keys[5], vec_pieces), NV_PAD),
        'moment_vec': moment_draw(keys[6], NV_PAD, VEC_COUNT),
        'second_vec': second_draw(keys[7], NV_PAD, VEC_COUNT),
    }


def row_total(grad_block):
    def add_row(running, row_vals):
        return running + row_vals.astype(jnp.float32), None

    total, _ = lax.scan(add_row, jnp.zeros(grad_block.shape[1:], jnp.float32), grad_block)
    return total


def adam_update(grad_sum, clip_coef, master, moment, second, decay):
    clip_grad = clip_coef * grad_sum
    new_moment = BETA_ONE * moment + (1.0 - BETA_ONE) * clip_grad
    new_second = BETA_TWO * second + (1.0 - BETA_TWO) * clip_grad * clip_grad
    step_dir = (new_moment / FIX_ONE) / (jnp.sqrt(new_second / FIX_TWO) + ADAM_EPS)
    new_master = master - LEARN_RATE * (step_dir + decay * master)
    return new_master, new_moment, new_second


def reference(grad_mat, grad_vec, master_mat, moment_mat, second_mat, master_vec, moment_vec, second_vec):
    sum_mat = row_total(grad_mat)
    sum_vec = row_total(grad_vec)
    total_norm = jnp.sqrt(jnp.sum(sum_mat * sum_mat) + jnp.sum(sum_vec * sum_vec))
    clip_coef = jnp.minimum(1.0, 1.0 / (total_norm + NORM_EPS))
    mat_out = adam_update(sum_mat, clip_coef, master_mat, moment_mat, second_mat, DECAY)
    vec_out = adam_update(sum_vec, clip_coef, master_vec, moment_vec, second_vec, 0.0)
    return (mat_out[0], mat_out[1], mat_out[2], vec_out[0], vec_out[1], vec_out[2],
            mat_out[0].astype(jnp.bfloat16), vec_out[0].astype(jnp.bfloat16))
```

```python
import functools

import jax
import jax.numpy as jnp
from jax import lax
from jax.experimental import pallas as pl
from jax.experimental.pallas import tpu as pltpu
from jax.sharding import PartitionSpec as P

STEP = 4
LEARN_RATE = 1e-3
BETA_ONE = 0.9
BETA_TWO = 0.999
ADAM_EPS = 1e-8
DECAY = 0.01
NORM_EPS = 1e-6
FIX_ONE = 1.0 - BETA_ONE ** STEP
FIX_TWO = 1.0 - BETA_TWO ** STEP

MESH = pl.DeviceIdType.MESH
LANES = 128
BLK = 80
CHUNKS = 20
ADAM_ROWS = 720
SPLITS = (5, 27, 8)
VMEM_MAX = 64 * 1024 * 1024 - 64 * 1024


def adam_update(grad_sum, clip_coef, master, moment, second, decay):
    clip_grad = clip_coef * grad_sum
    new_moment = BETA_ONE * moment + (1.0 - BETA_ONE) * clip_grad
    new_second = BETA_TWO * second + (1.0 - BETA_TWO) * clip_grad * clip_grad
    step_dir = (new_moment / FIX_ONE) / (jnp.sqrt(new_second / FIX_TWO) + ADAM_EPS)
    new_master = master - LEARN_RATE * (step_dir + decay * master)
    return new_master, new_moment, new_second


def remote(src, dst, send_sem, recv_sem, dev):
    return pltpu.make_async_remote_copy(src_ref=src, dst_ref=dst, send_sem=send_sem, recv_sem=recv_sem,
                                        device_id=(dev,), device_id_type=MESH)


def scatter_kernel(share, rows, chunks, graw, vraw, g_out, gv_out, c_out,
                   raw, send_p, send_x, send_y, own, recv_p, recv_x, recv_y, part_s, part_r, total,
                   vbuf, vsend, vall, nsend, nall, acc,
                   load_sem, out_sem, sp_sem, sx_sem, sy_sem, rp_sem, rx_sem, ry_sem, ps_sem, pr_sem,
                   free_sem, pfree_sem, vload_sem, vs_sem, vr_sem, ns_sem, nr_sem):
    me = lax.axis_index('fsdp')
    core, cx, cy = lax.rem(me, 2), lax.rem(me // 2, 2), me // 4
    mate, ox, oy = 1 - core, 1 - cx, 1 - cy

    def dev(y, x, c):
        return 4 * y + 2 * x + c

    half = share // 2
    width = rows * LANES

    barrier = pltpu.get_barrier_semaphore()
    for d in range(1, 8):
        pl.semaphore_signal(barrier, inc=1, device_id=(lax.rem(me + d, 8),), device_id_type=MESH)

    pieces = []
    for j in range(2):
        pieces += [(dev(cy, ox, j), 0), (dev(oy, ox, j), 0)]
    for j in range(2):
        pieces += [(dev(oy, cx, j), 1), (dev(oy, ox, j), 1)]
    for c in (mate, core):
        pieces += [(dev(cy, cx, c), 0), (dev(oy, cx, c), 0), (dev(cy, cx, c), 1), (dev(cy, ox, c), 1)]

    def start_load(t, slot):
        for q, (s, h) in enumerate(pieces):
            off = pl.multiple_of((s * share + h * half + t * rows) * LANES, 2048)
            pltpu.make_async_copy(graw.at[:, pl.ds(off, width)], raw.at[slot, :, pl.ds(q * width, width)],
                                  load_sem.at[slot]).start()

    def wait_load(slot):
        pltpu.make_async_copy(graw.at[:, pl.ds(0, 16 * width)], raw.at[slot], load_sem.at[slot]).wait()

    def squeeze(slot, q, dst, base):
        def body(i, carry):
            col = pl.multiple_of(q * width + i * (BLK * LANES), 2048)
            vals = raw[slot, :, pl.ds(col, BLK * LANES)].astype(jnp.float32).reshape(BLK, LANES)
            dst[pl.ds(pl.multiple_of(base + i * BLK, 16), BLK), :] = vals.astype(jnp.bfloat16)
            return carry
        lax.fori_loop(0, rows // BLK, body, 0)

    def copies(slot):
        out = []
        for j in range(2):
            out.append(remote(send_x.at[slot, j], recv_x.at[slot, core], sx_sem.at[slot, j], rx_sem.at[slot, core],
                              dev(cy, ox, j)))
            out.append(remote(send_y.at[slot, j], recv_y.at[slot, core], sy_sem.at[slot, j], ry_sem.at[slot, core],
                              dev(oy, cx, j)))
        out.append(remote(send_p.at[slot], recv_p.at[slot], sp_sem.at[slot], rp_sem.at[slot], dev(cy, cx, mate)))
        return out

    def wait_arrivals(slot):
        for j in range(2):
            remote(send_x.at[slot, j], recv_x.at[slot, j], sx_sem.at[slot, j], rx_sem.at[slot, j],
                   dev(cy, ox, j)).wait_recv()
            remote(send_y.at[slot, j], recv_y.at[slot, j], sy_sem.at[slot, j], ry_sem.at[slot, j],
                   dev(oy, cx, j)).wait_recv()
        remote(send_p.at[slot], recv_p.at[slot], sp_sem.at[slot], rp_sem.at[slot], dev(cy, cx, mate)).wait_recv()

    def part_copies(slot):
        return [remote(part_s.at[slot, 0], part_r.at[slot, 0], ps_sem.at[slot, 0], pr_sem.at[slot, 0],
                       dev(oy, cx, core)),
                remote(part_s.at[slot, 1], part_r.at[slot, 1], ps_sem.at[slot, 1], pr_sem.at[slot, 1],
                       dev(cy, ox, core))]

    def out_copies(t, slot):
        return [pltpu.make_async_copy(total.at[slot, h],
                                      g_out.at[pl.ds(pl.multiple_of(h * half + t * rows, 16), rows), :],
                                      out_sem.at[slot, h]) for h in range(2)]

    def give_credit():
        pl.semaphore_signal(free_sem.at[0], inc=1, device_id=(dev(cy, cx, mate),), device_id_type=MESH)
        for j in range(2):
            pl.semaphore_signal(free_sem.at[1 + core], inc=1, device_id=(dev(cy, ox, j),), device_id_type=MESH)
            pl.semaphore_signal(free_sem.at[3 + core], inc=1, device_id=(dev(oy, cx, j),), device_id_type=MESH)

    def four_sum(slot, h, k, dst):
        far = recv_x if h == 0 else recv_y
        q = 2 * h + k

        def body(i, carry):
            at = pl.ds(pl.multiple_of(q * rows + i * BLK, 16), BLK)
            fat = pl.ds(pl.multiple_of(k * rows + i * BLK, 16), BLK)
            vals = (own[slot, at, :].astype(jnp.float32) + recv_p[slot, at, :].astype(jnp.float32)
                    + far[slot, 0, fat, :].astype(jnp.float32) + far[slot, 1, fat, :].astype(jnp.float32))
            dst[slot, h, pl.ds(pl.multiple_of(i * BLK, 16), BLK), :] = vals
            return carry
        lax.fori_loop(0, rows // BLK, body, 0)

    start_load(0, 0)
    vload = pltpu.make_async_copy(vraw, vbuf, vload_sem)
    vload.start()
    acc[...] = jnp.zeros_like(acc)
    vload.wait()
    vec_bf = vbuf[...].astype(jnp.float32).reshape(vsend.shape).astype(jnp.bfloat16)
    vsend[...] = vec_bf
    vall[me] = vec_bf
    pl.semaphore_wait(barrier, 7)

    def vec_copy(d):
        return remote(vsend, vall.at[me], vs_sem.at[d], vr_sem.at[me], lax.rem(me + d, 8))

    for d in range(1, 8):
        vec_copy(d).start()

    def step(i, carry):
        slot, prev = lax.rem(i, 2), lax.rem(i + 1, 2)

        @pl.when(i + 1 < chunks)
        def _():
            start_load(i + 1, prev)

        @pl.when(i < chunks)
        def _():
            wait_load(slot)

            @pl.when(i >= 2)
            def _():
                for copy in copies(slot):
                    copy.wait_send()

            for j in range(2):
                for k in range(2):
                    squeeze(slot, 2 * j + k, send_x.at[slot, j], k * rows)
                    squeeze(slot, 4 + 2 * j + k, send_y.at[slot, j], k * rows)
            for q in range(4):
                squeeze(slot, 8 + q, send_p.at[slot], q * rows)
            for q in range(4):
                squeeze(slot, 12 + q, own.at[slot], q * rows)

            @pl.when(i >= 2)
            def _():
                for n in range(5):
                    pl.semaphore_wait(free_sem.at[n], 1)

            for copy in copies(slot):
                copy.start()

        @pl.when((i >= 1) & (i <= chunks))
        def _():
            wait_arrivals(prev)

            @pl.when(i >= 3)
            def _():
                for copy in part_copies(prev):
                    copy.wait_send()
                for n in range(2):
                    pl.semaphore_wait(pfree_sem.at[n], 1)
                for copy in out_copies(i - 3, prev):
                    copy.wait()

            four_sum(prev, 0, 1, part_s)
            four_sum(prev, 1, 1, part_s)
            four_sum(prev, 0, 0, total)
            four_sum(prev, 1, 0, total)
            for copy in part_copies(prev):
                copy.start()

            @pl.when(i - 1 < chunks - 2)
            def _():
                give_credit()

        @pl.when(i >= 2)
        def _():
            for copy in part_copies(slot):
                copy.wait_recv()
            for h in range(2):
                def body(n, run):
                    at = pl.ds(pl.multiple_of(n * BLK, 16), BLK)
                    vals = total[slot, h, at, :] + part_r[slot, h, at, :]
                    total[slot, h, at, :] = vals
                    return run + jnp.sum((vals * vals).reshape(BLK // 8, 8, LANES), axis=0)
                acc[...] += lax.fori_loop(0, rows // BLK, body, jnp.zeros((8, LANES), jnp.float32))
            for copy in out_copies(i - 2, slot):
                copy.start()

            @pl.when(i - 2 < chunks - 2)
            def _():
                pl.semaphore_signal(pfree_sem.at[0], inc=1, device_id=(dev(oy, cx, core),), device_id_type=MESH)
                pl.semaphore_signal(pfree_sem.at[1], inc=1, device_id=(dev(cy, ox, core),), device_id_type=MESH)
        return carry

    lax.fori_loop(0, chunks + 2, step, 0)

    nsend[...] = acc[...]
    nall[me] = acc[...]

    def norm_copy(d):
        return remote(nsend, nall.at[me], ns_sem.at[d], nr_sem.at[me], lax.rem(me + d, 8))

    for d in range(1, 8):
        j = lax.rem(me + d, 8)
        remote(vsend, vall.at[j], vs_sem.at[d], vr_sem.at[j], j).wait_recv()
    vec_sum = vall[0].astype(jnp.float32)
    for j in range(1, 8):
        vec_sum = vec_sum + vall[j].astype(jnp.float32)
    gv_out[...] = vec_sum
    square = jnp.sum((vec_sum * vec_sum).reshape(-1, 8, LANES), axis=0)
    for d in range(1, 8):
        norm_copy(d).start()
    for d in range(1, 8):
        j = lax.rem(me + d, 8)
        remote(nsend, nall.at[j], ns_sem.at[d], nr_sem.at[j], j).wait_recv()
    for j in range(8):
        square = square + nall[j]
    total_norm = jnp.sqrt(jnp.full((8, LANES), jnp.sum(square), jnp.float32))
    c_out[...] = jnp.minimum(1.0, 1.0 / (total_norm + NORM_EPS))

    for t in (chunks - 2, chunks - 1):
        for copy in copies(t % 2):
            copy.wait_send()
        for copy in part_copies(t % 2):
            copy.wait_send()
        for copy in out_copies(t, t % 2):
            copy.wait()
    for d in range(1, 8):
        vec_copy(d).wait_send()
        norm_copy(d).wait_send()


def reduce_grads(grad_mat, grad_vec):
    share = grad_mat.shape[1] // 8 // LANES
    vrows = grad_vec.shape[1] // LANES
    rows = share // 2 // CHUNKS
    bf, f32 = jnp.bfloat16, jnp.float32
    vm, dma = pltpu.VMEM, pltpu.SemaphoreType.DMA
    scratch = [
        vm((2, 1, 16 * rows * LANES), bf),
        vm((2, 4 * rows, LANES), bf), vm((2, 2, 2 * rows, LANES), bf), vm((2, 2, 2 * rows, LANES), bf),
        vm((2, 4 * rows, LANES), bf),
        vm((2, 4 * rows, LANES), bf), vm((2, 2, 2 * rows, LANES), bf), vm((2, 2, 2 * rows, LANES), bf),
        vm((2, 2, rows, LANES), f32), vm((2, 2, rows, LANES), f32), vm((2, 2, rows, LANES), f32),
        vm((1, vrows * LANES), bf), vm((vrows, LANES), bf), vm((8, vrows, LANES), bf),
        vm((8, LANES), f32), vm((8, 8, LANES), f32), vm((8, LANES), f32),
        dma((2,)), dma((2, 2)), dma((2,)), dma((2, 2)), dma((2, 2)), dma((2,)), dma((2, 2)), dma((2, 2)),
        dma((2, 2)), dma((2, 2)),
        pltpu.SemaphoreType.REGULAR((5,)), pltpu.SemaphoreType.REGULAR((2,)),
        dma, dma((8,)), dma((8,)), dma((8,)), dma((8,)),
    ]
    hbm = pl.BlockSpec(memory_space=pl.ANY)
    vmem = pl.BlockSpec(memory_space=pltpu.VMEM)
    return pl.pallas_call(
        functools.partial(scatter_kernel, share, rows, CHUNKS),
        out_shape=(jax.ShapeDtypeStruct((share, LANES), f32), jax.ShapeDtypeStruct((vrows, LANES), f32),
                   jax.ShapeDtypeStruct((8, LANES), f32)),
        in_specs=[hbm, hbm], out_specs=(hbm, vmem, vmem),
        scratch_shapes=scratch,
        compiler_params=pltpu.CompilerParams(collective_id=0, has_side_effects=True, vmem_limit_bytes=VMEM_MAX),
        name='reduce_grads',
    )(grad_mat, grad_vec)


def adam_kernel(c_ref, g_ref, p_ref, m_ref, v_ref, *refs):
    new_p, new_m, new_v, w_ref = refs[-4:]
    coef = c_ref[0:1, :]
    master, moment, second = adam_update(g_ref[...], coef, p_ref[...], m_ref[...], v_ref[...], DECAY)
    new_p[...] = master
    new_m[...] = moment
    new_v[...] = second
    w_ref[...] = master.astype(jnp.bfloat16)


def adam_part(first, count, coef, grads, master, moment, second, before):
    share = grads.shape[0]
    f32 = jnp.float32
    block = pl.BlockSpec((ADAM_ROWS, LANES), lambda i: (first + i, 0))
    extra = [] if before is None else list(before)
    elems = count * ADAM_ROWS * LANES
    return pl.pallas_call(
        adam_kernel,
        grid=(count,),
        out_shape=[jax.ShapeDtypeStruct((share, LANES), f32)] * 3
        + [jax.ShapeDtypeStruct((count * ADAM_ROWS, LANES), jnp.bfloat16)],
        in_specs=[pl.BlockSpec((8, LANES), lambda i: (0, 0))] + [block] * 4
        + [pl.BlockSpec(memory_space=pl.ANY)] * len(extra),
        out_specs=[block] * 3 + [pl.BlockSpec((ADAM_ROWS, LANES), lambda i: (i, 0))],
        input_output_aliases={5 + n: n for n in range(len(extra))},
        cost_estimate=pl.CostEstimate(flops=20 * elems, bytes_accessed=30 * elems, transcendentals=2 * elems),
        name='adam',
    )(coef, grads, master, moment, second, *extra)


def place_kernel(src_ref, *refs):
    refs[-1][...] = src_ref[...]


def place_part(first, count, share, part, before):
    blocks = share // ADAM_ROWS
    extra = [] if before is None else [before]
    elems = 8 * count * ADAM_ROWS * LANES
    return pl.pallas_call(
        place_kernel,
        grid=(8, count),
        out_shape=jax.ShapeDtypeStruct((8 * share, LANES), jnp.bfloat16),
        in_specs=[pl.BlockSpec((ADAM_ROWS, LANES), lambda d, i: (d * count + i, 0))]
        + [pl.BlockSpec(memory_space=pl.ANY)] * len(extra),
        out_specs=pl.BlockSpec((ADAM_ROWS, LANES), lambda d, i: (d * blocks + first + i, 0)),
        input_output_aliases={1 + n: n for n in range(len(extra))},
        cost_estimate=pl.CostEstimate(flops=elems, bytes_accessed=4 * elems, transcendentals=0),
        name='place',
    )(part, *extra)


def solution(mesh):
    def local_step(grad_mat, grad_vec, master_mat, moment_mat, second_mat, master_vec, moment_vec, second_vec):
        grads, vec_sum, coef = reduce_grads(grad_mat, grad_vec)
        share = grads.shape[0]
        state = [a.reshape(share, LANES) for a in (master_mat, moment_mat, second_mat)]
        first, new_mat, gathered = 0, None, []
        for count in SPLITS:
            *new_mat, part = adam_part(first, count, coef, grads, *state, new_mat)
            gathered.append(lax.all_gather(part.reshape(-1), 'fsdp', tiled=True))
            first += count
        first, weights = 0, None
        for count, part in zip(SPLITS, gathered):
            weights = place_part(first, count, share, part.reshape(-1, LANES), weights)
            first += count

        vshare = master_vec.shape[0]
        my_vec = lax.dynamic_slice(vec_sum.reshape(-1), (lax.axis_index('fsdp') * vshare,), (vshare,))
        new_vec = adam_update(my_vec, coef[0, 0], master_vec, moment_vec, second_vec, 0.0)
        weights_vec = lax.all_gather(new_vec[0].astype(jnp.bfloat16), 'fsdp', tiled=True)
        return tuple(a.reshape(-1) for a in new_mat) + new_vec + (weights.reshape(-1), weights_vec)

    row_spec = P('fsdp', None)
    flat_spec = P('fsdp')
    whole_spec = P()
    return jax.shard_map(local_step, mesh=mesh,
                         in_specs=(row_spec, row_spec) + (flat_spec,) * 6,
                         out_specs=(flat_spec,) * 6 + (whole_spec, whole_spec),
                         check_vma=False)
```
